32 devices in a mesh: tp: 8 (over y, x, core), col: 4 (over z).
Axes of the slice: x: 2, y: 2, z: 4, core: 2. Of those that a mesh axis runs over, the one named last changes fastest.
Arguments:
- gate_in: bfloat16 [128, 53248], P('col', 'tp'), may hold values from -6 to 6
- up_in: bfloat16 [128, 53248], P('col', 'tp'), may hold values from -6 to 6
- down_weight: bfloat16 [53248, 16384], P('tp', 'col'), may hold values from -0.02734375 to 0.02734375
- residual: bfloat16 [128, 16384], P('tp', 'col'), may hold values from -30 to 30
- norm_gain: bfloat16 [16384], P('col'), may hold values from 0.5 to 1.5
Outputs:
- stream: bfloat16 [128, 16384], P('tp', 'col')
- normed: bfloat16 [128, 16384], P('tp', 'col')
The draws below stay inside these ranges and needn't reach their ends.
All inputs are finite; a program needn't handle non-finite values.
Results may differ from the reference program's by a relative error of at most 0.0034.
Values may be sent and summed in bfloat16 or wider, within the bound.
A program may use at most 128 MiB of HBM per device.

```python
import math
import jax
import jax.numpy as jnp
from jax import lax

D = 16384
FF = 53248
TOKENS = 128


def draw_residual(key, part):
    key_rows = jax.random.fold_in(key, 11)
    key_values = jax.random.fold_in(key, 23)
    row_scale = jnp.exp(jax.random.uniform(key_rows, (TOKENS, 1), jnp.float32, math.log(0.3), math.log(3.0)))
    ramp = jnp.arange(D, dtype=jnp.float32) / (D - 1)
    col_scale = 0.5 * jnp.exp(ramp * math.log(3.0))
    values = jnp.clip(jax.random.normal(key_values, (TOKENS, D), jnp.float32), -4.0, 4.0)
    return (row_scale * col_scale[None, :] * values).astype(jnp.bfloat16)


def levels(stream_key, extent, shards, smallest, high):
    def one(position, parts):
        draws = jax.random.uniform(jax.random.fold_in(jax.random.fold_in(stream_key, 6), position), (parts,), jnp.float32, smallest / len(shards), high / len(shards))
        return jnp.repeat(jnp.exp(draws), extent[position] // parts).reshape((-1,) + (1,) * (len(extent) - position - 1))

    factor_of = one(*shards[0])
    for cut in shards[1:]:
        factor_of = factor_of * one(*cut)
    return factor_of


def noise(key, dims, scale, most, cuts=(), kind=jnp.bfloat16):
    drawn = scale * jax.random.normal(key, dims, jnp.float32)
    if cuts:
        drawn = drawn * levels(key, dims, cuts, -0.22, 0.18)
    return jnp.clip(drawn, -most, most).astype(kind)


def setup_inputs(seed: int = 0) -> dict:
    arg_keys = jax.random.split(jax.random.key(seed), 6)
    return {
        "gate_in": noise(arg_keys[0], (TOKENS, FF), 1.0, 6.0, ((0, 4), (1, 8))),
        "up_in": noise(arg_keys[1], (TOKENS, FF), 1.0, 6.0, ((0, 4), (1, 8))),
        "down_weight": noise(arg_keys[2], (FF, D), FF ** -0.5, 0.02734375, ((0, 8), (1, 4))),
        "residual": draw_residual(jax.random.fold_in(arg_keys[5], 71), 0),
        "norm_gain": jnp.clip(1.0 + 0.1 * jax.random.normal(arg_keys[4], (D,), jnp.float32), 0.5, 1.5).astype(jnp.bfloat16),
    }


def reference(gate_in, up_in, down_weight, residual, norm_gain):
    hidden = (jax.nn.silu(gate_in.astype(jnp.float32)) * up_in.astype(jnp.float32)).astype(jnp.bfloat16)
    branch = jnp.dot(hidden, down_weight, preferred_element_type=jnp.float32)
    summed = residual.astype(jnp.float32) + branch
    mean_square = lax.optimization_barrier(jnp.mean(summed * summed, axis=1, keepdims=True))
    scaled = summed * lax.rsqrt(mean_square + 1e-05) * norm_gain.astype(jnp.float32)[None, :]
    return (summed.astype(jnp.bfloat16), scaled.astype(jnp.bfloat16))
```

```python
import functools

import jax
import jax.numpy as jnp
from jax import lax
from jax.experimental import pallas as pl
from jax.experimental.pallas import tpu as pltpu
from jax.sharding import PartitionSpec as P

MESH = pl.DeviceIdType.MESH
VMEM_BYTES = 67_043_328
EPS = 1e-05


def gated(gate_part, up_part):
    return (jax.nn.silu(gate_part.astype(jnp.float32)) * up_part.astype(jnp.float32)).astype(
        jnp.bfloat16
    )


def plain_body(width, gate_in, up_in, down_weight, residual, norm_gain):
    local_act = gated(gate_in, up_in)
    hidden = lax.all_gather(local_act, "col", axis=0, tiled=True)
    partial_value = jnp.dot(hidden, down_weight, preferred_element_type=jnp.float32)
    branch = lax.psum_scatter(partial_value, "tp", scatter_dimension=0, tiled=True)
    summed = residual.astype(jnp.float32) + branch
    local_squares = jnp.sum(summed * summed, axis=1, keepdims=True)
    mean_square = lax.psum(local_squares, "col") / width
    scaled = summed * lax.rsqrt(mean_square + EPS) * norm_gain.astype(jnp.float32)[None, :]
    return (summed.astype(jnp.bfloat16), scaled.astype(jnp.bfloat16))


def pick(extent, most, step):
    best = 0
    for size in range(step, min(extent, most) + 1, step):
        if extent % size == 0:
            best = size
    return best


def kernel(
    n_col, n_pair, kp, nt, rt, skew,
    gate_hbm, up_hbm, w_hbm, res_hbm,
    out_hbm, sq_out,
    gate_v, up_v, hid, w_v, acc, peer, send_buf, recv_buf, own, res_v, total, squares,
    in_sem, w_sem, res_sem, out_sem, ag_send, ag_recv, d_send, d_recv, r_send, r_recv, q_send, q_recv,
):
    rows, depth = gate_hbm.shape
    width = w_hbm.shape[1]
    pieces = depth // kp
    tiles = width // rt
    me = lax.axis_index("tp")
    z = lax.axis_index("col")
    plane, core = me // 2, lax.rem(me, 2)

    barrier = pltpu.get_barrier_semaphore()
    for step in range(1, n_col):
        pl.semaphore_signal(
            barrier, inc=1, device_id={"col": lax.rem(z + step, n_col)}, device_id_type=MESH
        )
    pl.semaphore_signal(barrier, inc=1, device_id={"tp": 2 * plane + 1 - core}, device_id_type=MESH)
    for step in range(1, n_pair):
        pl.semaphore_signal(
            barrier,
            inc=1,
            device_id={"tp": 2 * lax.rem(plane + step, n_pair) + core},
            device_id_type=MESH,
        )

    def cols(s):
        return pl.ds(pl.multiple_of(s * kp, kp), kp)

    def load(s, which):
        src, dst = ((gate_hbm, gate_v), (up_hbm, up_v))[which]
        return pltpu.make_async_copy(src.at[:, cols(s)], dst.at[:, cols(s)], in_sem.at[which, s])

    def load_w(s):
        return pltpu.make_async_copy(w_hbm.at[cols(s), :], w_v.at[cols(s), :], w_sem.at[s])

    load_res = pltpu.make_async_copy(res_hbm, res_v, res_sem)

    @pl.loop(0, pieces)
    def _(s):
        load(s, 0).start()
        load(s, 1).start()

    @pl.loop(0, pieces)
    def _(s):
        load_w(s).start()

    load_res.start()

    def hid_rows(source):
        return pl.ds(pl.multiple_of(source * rows, rows), rows)

    def hop(source, s, up):
        block = hid.at[hid_rows(source), cols(s)]
        return pltpu.make_async_remote_copy(
            src_ref=block,
            dst_ref=block,
            send_sem=ag_send.at[0 if up else 1, source],
            recv_sem=ag_recv.at[source, s],
            device_id={"col": z + 1 if up else z - 1},
            device_id_type=MESH,
        )

    def send_both(source, s):
        @pl.when(z < n_col - 1)
        def _():
            hop(source, s, True).start()

        @pl.when(z > 0)
        def _():
            hop(source, s, False).start()

    pl.semaphore_wait(barrier, n_col - 1 + 1 + n_pair - 1)

    @pl.loop(0, pieces + 1)
    def _(s):
        @pl.when(s < pieces)
        def _():
            load(s, 0).wait()
            load(s, 1).wait()
            g = gate_v[:, cols(s)].astype(jnp.float32)
            u = up_v[:, cols(s)].astype(jnp.float32)
            hid[hid_rows(z), cols(s)] = (g / (1.0 + jnp.exp(-g)) * u).astype(jnp.bfloat16)

        @pl.when(s > 0)
        def _():
            send_both(z, s - 1)

    acc[...] = jnp.zeros_like(acc)

    @pl.loop(0, pieces + skew * (n_col - 2))
    def _(i):
        for away in range(n_col - 1, 0, -1):
            s = i - skew * (away - 1)
            live = jnp.logical_and(s >= 0, s < pieces)

            @pl.when(jnp.logical_and(live, z - away >= 0))
            def _():
                hop(z - away, s, True).wait_recv()

                @pl.when(z < n_col - 1)
                def _():
                    hop(z - away, s, True).start()

            @pl.when(jnp.logical_and(live, z + away < n_col))
            def _():
                hop(z + away, s, False).wait_recv()

                @pl.when(z > 0)
                def _():
                    hop(z + away, s, False).start()

        s = i - skew * (n_col - 2)

        @pl.when(s >= 0)
        def _():
            load_w(s).wait()
            a = hid[:, cols(s)]
            for n in range(width // nt):
                part = jnp.dot(
                    a, w_v[cols(s), n * nt : (n + 1) * nt], preferred_element_type=jnp.float32
                )
                acc[:, :, :, n * nt : (n + 1) * nt] += part.reshape(acc.shape[:3] + (nt,))

    def swap(n):
        return pltpu.make_async_remote_copy(
            src_ref=acc.at[:, 1 - core, :, n * rt : (n + 1) * rt],
            dst_ref=peer.at[:, :, n * rt : (n + 1) * rt],
            send_sem=d_send,
            recv_sem=d_recv.at[n],
            device_id={"tp": 2 * plane + 1 - core},
            device_id_type=MESH,
        )

    def scatter(n, step):
        to = lax.rem(plane + step, n_pair)
        return pltpu.make_async_remote_copy(
            src_ref=send_buf.at[to, :, n * rt : (n + 1) * rt],
            dst_ref=recv_buf.at[step - 1, :, n * rt : (n + 1) * rt],
            send_sem=r_send.at[step - 1],
            recv_sem=r_recv.at[step - 1, n],
            device_id={"tp": 2 * to + core},
            device_id_type=MESH,
        )

    for n in range(tiles):
        swap(n).start()
    load_res.wait()
    for n in range(tiles + 1):
        if n < tiles:
            here = slice(n * rt, (n + 1) * rt)
            swap(n).wait_recv()
            both = acc[:, core, :, here] + peer[:, :, here]
            send_buf[:, :, here] = both.astype(jnp.bfloat16)
            own[:, here] = (
                acc[plane, core, :, here] + peer[plane, :, here]
                + res_v[:, here].astype(jnp.float32)
            )
        if n > 0:
            for step in range(1, n_pair):
                scatter(n - 1, step).start()

    sums = jnp.zeros((res_hbm.shape[0], 128), jnp.float32)
    writes = []
    for n in range(tiles):
        here = slice(n * rt, (n + 1) * rt)
        value = own[:, here]
        for step in range(1, n_pair):
            scatter(n, step).wait_recv()
            value = value + recv_buf[step - 1, :, here].astype(jnp.float32)
        total[:, here] = value
        square = value * value
        for j in range(rt // 128):
            sums = sums + square[:, j * 128 : (j + 1) * 128]
        write = pltpu.make_async_copy(total.at[:, here], out_hbm.at[:, here], out_sem.at[n])
        write.start()
        writes.append(write)

    squares[z] = jnp.broadcast_to(jnp.sum(sums, axis=1, keepdims=True), sums.shape)

    def share(step):
        return pltpu.make_async_remote_copy(
            src_ref=squares.at[z],
            dst_ref=squares.at[z],
            send_sem=q_send.at[step - 1],
            recv_sem=q_recv.at[step - 1],
            device_id={"col": lax.rem(z + step, n_col)},
            device_id_type=MESH,
        )

    def arrival(step):
        block = squares.at[lax.rem(z + n_col - step, n_col)]
        return pltpu.make_async_remote_copy(
            src_ref=block,
            dst_ref=block,
            send_sem=q_send.at[step - 1],
            recv_sem=q_recv.at[step - 1],
            device_id={"col": lax.rem(z + step, n_col)},
            device_id_type=MESH,
        )

    for step in range(1, n_col):
        share(step).start()

    for source in range(n_col):
        block = hid.at[source * rows : (source + 1) * rows, :]
        for up in (0, 1):
            sent = jnp.logical_and(source <= z, z < n_col - 1)
            if not up:
                sent = jnp.logical_and(source >= z, z > 0)

            @pl.when(sent)
            def _():
                pltpu.make_async_remote_copy(
                    src_ref=block,
                    dst_ref=block,
                    send_sem=ag_send.at[0 if up else 1, source],
                    recv_sem=ag_recv.at[source, 0],
                    device_id={"col": z + 1 if up else z - 1},
                    device_id_type=MESH,
                ).wait_send()

    pltpu.make_async_remote_copy(
        src_ref=peer,
        dst_ref=peer,
        send_sem=d_send,
        recv_sem=d_recv.at[0],
        device_id={"tp": 2 * plane + 1 - core},
        device_id_type=MESH,
    ).wait_send()
    for step in range(1, n_pair):
        to = lax.rem(plane + step, n_pair)
        pltpu.make_async_remote_copy(
            src_ref=send_buf.at[to],
            dst_ref=recv_buf.at[step - 1],
            send_sem=r_send.at[step - 1],
            recv_sem=r_recv.at[step - 1, 0],
            device_id={"tp": 2 * to + core},
            device_id_type=MESH,
        ).wait_send()
    for write in writes:
        write.wait()
    for step in range(1, n_col):
        share(step).wait_send()
        arrival(step).wait_recv()
    whole = squares[0]
    for j in range(1, n_col):
        whole = whole + squares[j]
    sq_out[...] = whole


def fused_body(n_tp, n_col, kp, nt, rt, width, gate_in, up_in, down_weight, residual, norm_gain):
    rows, depth = gate_in.shape
    local = down_weight.shape[1]
    own_rows = residual.shape[0]
    n_pair = n_tp // 2
    pieces, tiles = depth // kp, local // rt
    any_space = pl.BlockSpec(memory_space=pl.ANY)
    dma = pltpu.SemaphoreType.DMA
    summed, squares = pl.pallas_call(
        functools.partial(kernel, n_col, n_pair, kp, nt, rt, min(3, pieces)),
        out_shape=(
            jax.ShapeDtypeStruct((own_rows, local), jnp.float32),
            jax.ShapeDtypeStruct((own_rows, 128), jnp.float32),
        ),
        in_specs=[any_space] * 4,
        out_specs=(any_space, pl.BlockSpec(memory_space=pltpu.VMEM)),
        scratch_shapes=[
            pltpu.VMEM((rows, depth), jnp.bfloat16),
            pltpu.VMEM((rows, depth), jnp.bfloat16),
            pltpu.VMEM((rows * n_col, depth), jnp.bfloat16),
            pltpu.VMEM((depth, local), jnp.bfloat16),
            pltpu.VMEM((n_pair, 2, own_rows, local), jnp.float32),
            pltpu.VMEM((n_pair, own_rows, local), jnp.float32),
            pltpu.VMEM((n_pair, own_rows, local), jnp.bfloat16),
            pltpu.VMEM((n_pair - 1, own_rows, local), jnp.bfloat16),
            pltpu.VMEM((own_rows, local), jnp.float32),
            pltpu.VMEM((own_rows, local), jnp.bfloat16),
            pltpu.VMEM((own_rows, local), jnp.float32),
            pltpu.VMEM((n_col, own_rows, 128), jnp.float32),
            dma((2, pieces)),
            dma((pieces,)),
            dma,
            dma((tiles,)),
            dma((2, n_col)),
            dma((n_col, pieces)),
            dma,
            dma((tiles,)),
            dma((n_pair - 1,)),
            dma((n_pair - 1, tiles)),
            dma((n_col - 1,)),
            dma((n_col - 1,)),
        ],
        compiler_params=pltpu.CompilerParams(
            collective_id=0, has_side_effects=True, vmem_limit_bytes=VMEM_BYTES
        ),
        name="down_reduce",
    )(gate_in, up_in, down_weight, residual)
    mean_square = squares[:, :1] / width
    scaled = summed * lax.rsqrt(mean_square + EPS) * norm_gain.astype(jnp.float32)[None, :]
    return (summed.astype(jnp.bfloat16), scaled.astype(jnp.bfloat16))


def pairs_share_chip(mesh):
    if tuple(mesh.axis_names) != ("tp", "col") or mesh.shape["tp"] % 2 or mesh.shape["tp"] < 4:
        return False
    devices = mesh.devices
    for j in range(0, mesh.shape["tp"], 2):
        for a, b in zip(devices[j], devices[j + 1]):
            first = getattr(a, "coords", None)
            if first is None or list(first) != list(getattr(b, "coords", ())):
                return False
    return True


def solution(mesh):
    in_specs = (P("col", "tp"), P("col", "tp"), P("tp", "col"), P("tp", "col"), P("col"))
    out_specs = (P("tp", "col"), P("tp", "col"))
    n_tp, n_col = mesh.shape["tp"], mesh.shape["col"]

    def run(gate_in, up_in, down_weight, residual, norm_gain):
        tokens, hidden_units = gate_in.shape
        width = down_weight.shape[1]
        depth, local = hidden_units // n_tp, width // n_col
        rows, own_rows = tokens // n_col, tokens // n_tp
        kp, nt, rt = pick(depth, 512, 128), pick(local, 1024, 128), pick(local, 512, 128)
        need = 2 * depth * (local + tokens + 2 * rows) + local * tokens * 9 + (4 << 20)
        fused = (
            pairs_share_chip(mesh)
            and n_col > 1
            and rows % 16 == 0
            and own_rows % 16 == 0
            and kp > 0
            and nt > 0
            and need < VMEM_BYTES
        )
        body = functools.partial(plain_body, width)
        if fused:
            body = functools.partial(fused_body, n_tp, n_col, kp, nt, rt, width)
        return jax.shard_map(
            body, mesh=mesh, in_specs=in_specs, out_specs=out_specs, check_vma=False
        )(gate_in, up_in, down_weight, residual, norm_gain)

    return run
```

```python
import functools

import jax
import jax.numpy as jnp
from jax import lax
from jax.experimental import pallas as pl
from jax.experimental.pallas import tpu as pltpu
from jax.sharding import PartitionSpec as P

MESH = pl.DeviceIdType.MESH
VMEM_BYTES = 67_043_328
EPS = 1e-05


def gated(gate_part, up_part):
    return (jax.nn.silu(gate_part.astype(jnp.float32)) * up_part.astype(jnp.float32)).astype(
        jnp.bfloat16
    )


def plain_body(width, gate_in, up_in, down_weight, residual, norm_gain):
    local_act = gated(gate_in, up_in)
    hidden = lax.all_gather(local_act, "col", axis=0, tiled=True)
    partial_value = jnp.dot(hidden, down_weight, preferred_element_type=jnp.float32)
    branch = lax.psum_scatter(partial_value, "tp", scatter_dimension=0, tiled=True)
    summed = residual.astype(jnp.float32) + branch
    local_squares = jnp.sum(summed * summed, axis=1, keepdims=True)
    mean_square = lax.psum(local_squares, "col") / width
    scaled = summed * lax.rsqrt(mean_square + EPS) * norm_gain.astype(jnp.float32)[None, :]
    return (summed.astype(jnp.bfloat16), scaled.astype(jnp.bfloat16))


def pick(extent, most, step):
    best = 0
    for size in range(step, min(extent, most) + 1, step):
        if extent % size == 0:
            best = size
    return best


def kernel(
    n_col, n_pair, kp, nt, rt, skew, d_model,
    gate_hbm, up_hbm, w_hbm, res_hbm,
    out_hbm, scale_out,
    gate_v, up_v, hid, w_v, acc, peer, send_buf, recv_buf, own, res_v, total, squares,
    in_sem, w_sem, res_sem, out_sem, ag_send, ag_recv, d_send, d_recv, r_send, r_recv, q_send, q_recv,
):
    rows, depth = gate_hbm.shape
    width = w_hbm.shape[1]
    pieces = depth // kp
    tiles = width // rt
    me = lax.axis_index("tp")
    z = lax.axis_index("col")
    plane, core = me // 2, lax.rem(me, 2)

    barrier = pltpu.get_barrier_semaphore()
    for step in range(1, n_col):
        pl.semaphore_signal(
            barrier, inc=1, device_id={"col": lax.rem(z + step, n_col)}, device_id_type=MESH
        )
    pl.semaphore_signal(barrier, inc=1, device_id={"tp": 2 * plane + 1 - core}, device_id_type=MESH)
    for step in range(1, n_pair):
        pl.semaphore_signal(
            barrier,
            inc=1,
            device_id={"tp": 2 * lax.rem(plane + step, n_pair) + core},
            device_id_type=MESH,
        )

    def cols(s):
        return pl.ds(pl.multiple_of(s * kp, kp), kp)

    def load(s, which):
        src, dst = ((gate_hbm, gate_v), (up_hbm, up_v))[which]
        return pltpu.make_async_copy(src.at[:, cols(s)], dst.at[:, cols(s)], in_sem.at[which, s])

    def load_w(s):
        return pltpu.make_async_copy(w_hbm.at[cols(s), :], w_v.at[cols(s), :], w_sem.at[s])

    load_res = pltpu.make_async_copy(res_hbm, res_v, res_sem)

    @pl.loop(0, pieces)
    def _(s):
        load(s, 0).start()
        load(s, 1).start()

    @pl.loop(0, pieces)
    def _(s):
        load_w(s).start()

    load_res.start()

    def hid_rows(source):
        return pl.ds(pl.multiple_of(source * rows, rows), rows)

    def hop(source, s, up):
        block = hid.at[hid_rows(source), cols(s)]
        return pltpu.make_async_remote_copy(
            src_ref=block,
            dst_ref=block,
            send_sem=ag_send.at[0 if up else 1, source],
            recv_sem=ag_recv.at[source, s],
            device_id={"col": z + 1 if up else z - 1},
            device_id_type=MESH,
        )

    def send_both(source, s):
        @pl.when(z < n_col - 1)
        def _():
            hop(source, s, True).start()

        @pl.when(z > 0)
        def _():
            hop(source, s, False).start()

    pl.semaphore_wait(barrier, n_col - 1 + 1 + n_pair - 1)

    @pl.loop(0, pieces + 1)
    def _(s):
        @pl.when(s < pieces)
        def _():
            load(s, 0).wait()
            load(s, 1).wait()
            g = gate_v[:, cols(s)].astype(jnp.float32)
            u = up_v[:, cols(s)].astype(jnp.float32)
            hid[hid_rows(z), cols(s)] = (g / (1.0 + jnp.exp(-g)) * u).astype(jnp.bfloat16)

        @pl.when(s > 0)
        def _():
            send_both(z, s - 1)

    acc[...] = jnp.zeros_like(acc)

    @pl.loop(0, pieces + skew * (n_col - 2))
    def _(i):
        for away in range(n_col - 1, 0, -1):
            s = i - skew * (away - 1)
            live = jnp.logical_and(s >= 0, s < pieces)

            @pl.when(jnp.logical_and(live, z - away >= 0))
            def _():
                hop(z - away, s, True).wait_recv()

                @pl.when(z < n_col - 1)
                def _():
                    hop(z - away, s, True).start()

            @pl.when(jnp.logical_and(live, z + away < n_col))
            def _():
                hop(z + away, s, False).wait_recv()

                @pl.when(z > 0)
                def _():
                    hop(z + away, s, False).start()

        s = i - skew * (n_col - 2)

        @pl.when(s >= 0)
        def _():
            load_w(s).wait()
            a = hid[:, cols(s)]
            for n in range(width // nt):
                part = jnp.dot(
                    a, w_v[cols(s), n * nt : (n + 1) * nt], preferred_element_type=jnp.float32
                )
                acc[:, :, :, n * nt : (n + 1) * nt] += part.reshape(acc.shape[:3] + (nt,))

    def swap(n):
        return pltpu.make_async_remote_copy(
            src_ref=acc.at[:, 1 - core, :, n * rt : (n + 1) * rt],
            dst_ref=peer.at[:, :, n * rt : (n + 1) * rt],
            send_sem=d_send,
            recv_sem=d_recv.at[n],
            device_id={"tp": 2 * plane + 1 - core},
            device_id_type=MESH,
        )

    def scatter(n, step):
        to = lax.rem(plane + step, n_pair)
        return pltpu.make_async_remote_copy(
            src_ref=send_buf.at[to, :, n * rt : (n + 1) * rt],
            dst_ref=recv_buf.at[step - 1, :, n * rt : (n + 1) * rt],
            send_sem=r_send.at[step - 1],
            recv_sem=r_recv.at[step - 1, n],
            device_id={"tp": 2 * to + core},
            device_id_type=MESH,
        )

    for n in range(tiles):
        swap(n).start()
    load_res.wait()
    for n in range(tiles + 1):
        if n < tiles:
            here = slice(n * rt, (n + 1) * rt)
            swap(n).wait_recv()
            both = acc[:, core, :, here] + peer[:, :, here]
            send_buf[:, :, here] = both.astype(jnp.bfloat16)
            own[:, here] = (
                acc[plane, core, :, here] + peer[plane, :, here]
                + res_v[:, here].astype(jnp.float32)
            )
        if n > 0:
            for step in range(1, n_pair):
                scatter(n - 1, step).start()

    sums = jnp.zeros((res_hbm.shape[0], 128), jnp.float32)
    writes = []
    for n in range(tiles):
        here = slice(n * rt, (n + 1) * rt)
        value = own[:, here]
        for step in range(1, n_pair):
            scatter(n, step).wait_recv()
            value = value + recv_buf[step - 1, :, here].astype(jnp.float32)
        total[:, here] = value
        square = value * value
        for j in range(rt // 128):
            sums = sums + square[:, j * 128 : (j + 1) * 128]
        write = pltpu.make_async_copy(total.at[:, here], out_hbm.at[:, here], out_sem.at[n])
        write.start()
        writes.append(write)

    squares[z] = jnp.broadcast_to(jnp.sum(sums, axis=1, keepdims=True), sums.shape)

    def share(step):
        return pltpu.make_async_remote_copy(
            src_ref=squares.at[z],
            dst_ref=squares.at[z],
            send_sem=q_send.at[step - 1],
            recv_sem=q_recv.at[step - 1],
            device_id={"col": lax.rem(z + step, n_col)},
            device_id_type=MESH,
        )

    def arrival(step):
        block = squares.at[lax.rem(z + n_col - step, n_col)]
        return pltpu.make_async_remote_copy(
            src_ref=block,
            dst_ref=block,
            send_sem=q_send.at[step - 1],
            recv_sem=q_recv.at[step - 1],
            device_id={"col": lax.rem(z + step, n_col)},
            device_id_type=MESH,
        )

    for step in range(1, n_col):
        share(step).start()

    for source in range(n_col):
        block = hid.at[source * rows : (source + 1) * rows, :]
        for up in (0, 1):
            sent = jnp.logical_and(source <= z, z < n_col - 1)
            if not up:
                sent = jnp.logical_and(source >= z, z > 0)

            @pl.when(sent)
            def _():
                pltpu.make_async_remote_copy(
                    src_ref=block,
                    dst_ref=block,
                    send_sem=ag_send.at[0 if up else 1, source],
                    recv_sem=ag_recv.at[source, 0],
                    device_id={"col": z + 1 if up else z - 1},
                    device_id_type=MESH,
                ).wait_send()

    pltpu.make_async_remote_copy(
        src_ref=peer,
        dst_ref=peer,
        send_sem=d_send,
        recv_sem=d_recv.at[0],
        device_id={"tp": 2 * plane + 1 - core},
        device_id_type=MESH,
    ).wait_send()
    for step in range(1, n_pair):
        to = lax.rem(plane + step, n_pair)
        pltpu.make_async_remote_copy(
            src_ref=send_buf.at[to],
            dst_ref=recv_buf.at[step - 1],
            send_sem=r_send.at[step - 1],
            recv_sem=r_recv.at[step - 1, 0],
            device_id={"tp": 2 * to + core},
            device_id_type=MESH,
        ).wait_send()
    for write in writes:
        write.wait()
    for step in range(1, n_col):
        share(step).wait_send()
        arrival(step).wait_recv()
    whole = squares[0]
    for j in range(1, n_col):
        whole = whole + squares[j]
    scale_out[...] = lax.rsqrt(whole / d_model + EPS)


def fused_body(n_tp, n_col, kp, nt, rt, width, gate_in, up_in, down_weight, residual, norm_gain):
    rows, depth = gate_in.shape
    local = down_weight.shape[1]
    own_rows = residual.shape[0]
    n_pair = n_tp // 2
    pieces, tiles = depth // kp, local // rt
    any_space = pl.BlockSpec(memory_space=pl.ANY)
    dma = pltpu.SemaphoreType.DMA
    summed, scale = pl.pallas_call(
        functools.partial(kernel, n_col, n_pair, kp, nt, rt, min(3, pieces), width),
        out_shape=(
            jax.ShapeDtypeStruct((own_rows, local), jnp.float32),
            jax.ShapeDtypeStruct((own_rows, 128), jnp.float32),
        ),
        in_specs=[any_space] * 4,
        out_specs=(any_space, pl.BlockSpec(memory_space=pltpu.VMEM)),
        scratch_shapes=[
            pltpu.VMEM((rows, depth), jnp.bfloat16),
            pltpu.VMEM((rows, depth), jnp.bfloat16),
            pltpu.VMEM((rows * n_col, depth), jnp.bfloat16),
            pltpu.VMEM((depth, local), jnp.bfloat16),
            pltpu.VMEM((n_pair, 2, own_rows, local), jnp.float32),
            pltpu.VMEM((n_pair, own_rows, local), jnp.float32),
            pltpu.VMEM((n_pair, own_rows, local), jnp.bfloat16),
            pltpu.VMEM((n_pair - 1, own_rows, local), jnp.bfloat16),
            pltpu.VMEM((own_rows, local), jnp.float32),
            pltpu.VMEM((own_rows, local), jnp.bfloat16),
            pltpu.VMEM((own_rows, local), jnp.float32),
            pltpu.VMEM((n_col, own_rows, 128), jnp.float32),
            dma((2, pieces)),
            dma((pieces,)),
            dma,
            dma((tiles,)),
            dma((2, n_col)),
            dma((n_col, pieces)),
            dma,
            dma((tiles,)),
            dma((n_pair - 1,)),
            dma((n_pair - 1, tiles)),
            dma((n_col - 1,)),
            dma((n_col - 1,)),
        ],
        compiler_params=pltpu.CompilerParams(
            collective_id=0, has_side_effects=True, vmem_limit_bytes=VMEM_BYTES
        ),
        name="down_reduce",
    )(gate_in, up_in, down_weight, residual)
    scaled = summed * scale[:, :1] * norm_gain.astype(jnp.float32)[None, :]
    return (summed.astype(jnp.bfloat16), scaled.astype(jnp.bfloat16))


def pairs_share_chip(mesh):
    if tuple(mesh.axis_names) != ("tp", "col") or mesh.shape["tp"] % 2 or mesh.shape["tp"] < 4:
        return False
    devices = mesh.devices
    for j in range(0, mesh.shape["tp"], 2):
        for a, b in zip(devices[j], devices[j + 1]):
            first = getattr(a, "coords", None)
            if first is None or list(first) != list(getattr(b, "coords", ())):
                return False
    return True


def solution(mesh):
    in_specs = (P("col", "tp"), P("col", "tp"), P("tp", "col"), P("tp", "col"), P("col"))
    out_specs = (P("tp", "col"), P("tp", "col"))
    n_tp, n_col = mesh.shape["tp"], mesh.shape["col"]

    def run(gate_in, up_in, down_weight, residual, norm_gain):
        tokens, hidden_units = gate_in.shape
        width = down_weight.shape[1]
        depth, local = hidden_units // n_tp, width // n_col
        rows, own_rows = tokens // n_col, tokens // n_tp
        kp, nt, rt = pick(depth, 512, 128), pick(local, 1024, 128), pick(local, 512, 128)
        need = 2 * depth * (local + tokens + 2 * rows) + local * tokens * 9 + (4 << 20)
        fused = (
            pairs_share_chip(mesh)
            and n_col > 1
            and rows % 16 == 0
            and own_rows % 16 == 0
            and kp > 0
            and nt > 0
            and need < VMEM_BYTES
        )
        body = functools.partial(plain_body, width)
        if fused:
            body = functools.partial(fused_body, n_tp, n_col, kp, nt, rt, width)
        return jax.shard_map(
            body, mesh=mesh, in_specs=in_specs, out_specs=out_specs, check_vma=False
        )(gate_in, up_in, down_weight, residual, norm_gain)

    return run
```
